32 devices in a mesh: kx: 4 (over y, x), ky: 8 (over z, core).
Axes of the slice: x: 2, y: 2, z: 4, core: 2. Of those that a mesh axis runs over, the one named last changes fastest.
Arguments:
- wannier: bfloat16 [16, 64, 64, 128], P('kx', 'ky'), may hold values from -0.5 to 0.5
- coupling: bfloat16 [3, 16, 64, 6, 64, 128], P(None, 'kx', 'ky'), may hold values from -6 to 6
- kq_map: int32 [3, 1024], replicated, may hold values from 0 to 1023, as said below
Outputs:
- rotated: bfloat16 [3, 16, 64, 6, 64, 128], P(None, 'kx', 'ky')
The draws below stay inside these ranges and needn't reach their ends.
Inputs may be any that keep to these rules, and one draw needn't show every extreme that they name: For every q there are offsets a and b with kq_map[q, x * 64 + y] = ((x + a) mod 16) * 64 + (y + b) mod 64.
All inputs are finite; a program needn't handle non-finite values.
Results may differ from the reference program's by a relative error of at most 0.0049.
Values may be sent and summed in bfloat16 or wider, within the bound.
A program may use at most 192 MiB of HBM per device.

```python
import jax
import jax.numpy as jnp

NB = 64
MODES = 6
Q = 3
KX_DEV = 4
KY_DEV = 8
NX = 16
NY = 64


def draw_kq_map(key, part):
    blocks_x = jax.random.randint(jax.random.fold_in(key, 11), (Q,), 0, NX // KX_DEV)
    blocks_x = blocks_x.at[0].set(NX // KX_DEV - 1)
    blocks_x = blocks_x.at[1].set(NX // KX_DEV // 2)
    blocks_y = jax.random.randint(jax.random.fold_in(key, 23), (Q,), 0, NY // KY_DEV)
    blocks_y = blocks_y.at[0].set(NY // KY_DEV - 1)
    blocks_y = blocks_y.at[1].set(NY // KY_DEV // 2)
    inner_x = jax.random.randint(jax.random.fold_in(key, 37), (Q,), 1, KX_DEV)
    inner_y = jax.random.randint(jax.random.fold_in(key, 41), (Q,), 1, KY_DEV)
    shift_x = blocks_x * KX_DEV + inner_x
    shift_y = blocks_y * KY_DEV + inner_y
    grid_x = jnp.arange(NX, dtype=jnp.int32)[None, :, None]
    grid_y = jnp.arange(NY, dtype=jnp.int32)[None, None, :]
    mapped = (grid_x + shift_x[:, None, None]) % NX * NY + (grid_y + shift_y[:, None, None]) % NY
    return mapped.reshape(Q, NX * NY).astype(jnp.int32)


def levels(own_key, dims, pieces, low, largest):
    def one(position, blocks):
        steps = jax.random.uniform(jax.random.fold_in(jax.random.fold_in(own_key, 6), position), (blocks,), jnp.float32, low / len(pieces), largest / len(pieces))
        return jnp.repeat(jnp.exp(steps), dims[position] // blocks).reshape((-1,) + (1,) * (len(dims) - position - 1))

    gain = one(*pieces[0])
    for cut in pieces[1:]:
        gain = gain * one(*cut)
    return gain


def centred(own_key, shape, spread, bound, cuts=(), kind=jnp.bfloat16):
    drawn = jax.random.normal(own_key, shape, jnp.float32) * spread
    if len(cuts) > 0:
        drawn = levels(own_key, shape, cuts, -0.22, 0.18) * drawn
    return jnp.clip(drawn, min=-bound, max=bound).astype(kind)


def setup_inputs(seed: int = 0) -> dict:
    key_list = jax.random.split(jax.random.key(seed), 4)
    return {
        "wannier": centred(key_list[0], (NX, NY, NB, 2 * NB), (2 * NB) ** -0.5, 0.5, ((0, 4), (1, 8))),
        "coupling": centred(key_list[1], (Q, NX, NY, MODES, NB, 2 * NB), 1.0, 6.0, ((1, 4), (2, 8))),
        "kq_map": draw_kq_map(jax.random.fold_in(key_list[3], 71), 0),
    }


def right_factor(matrix):
    half_width = matrix.shape[-1] // 2
    lower_half = jnp.concatenate([-matrix[..., half_width:], matrix[..., :half_width]], axis=-1)
    return jnp.concatenate([matrix, lower_half], axis=-2)


def rotate(block_g, factor, partner):
    half_width = partner.shape[-1] // 2
    half_turn = jnp.einsum("xymac,xycd->xymad", block_g.astype(jnp.float32), factor.astype(jnp.float32)).astype(jnp.bfloat16)
    stacked = jnp.concatenate([half_turn, jnp.concatenate([half_turn[..., half_width:], -half_turn[..., :half_width]], axis=-1)], axis=-2)
    partner_rows = jnp.concatenate([partner[..., :half_width], partner[..., half_width:]], axis=-2)
    return jnp.einsum("xyca,xymcd->xymad", partner_rows.astype(jnp.float32), stacked.astype(jnp.float32)).astype(jnp.bfloat16)


def reference(wannier, coupling, kq_map):
    factor = right_factor(wannier)
    flattened = wannier.reshape(NX * NY, NB, 2 * NB)
    results = []
    for qpoint in range(Q):
        partner = flattened[kq_map[qpoint]].reshape(NX, NY, NB, 2 * NB)
        results.append(rotate(coupling[qpoint], factor, partner))
    return jnp.stack(results, axis=0)
```

```python
import functools
import math

import jax
import jax.numpy as jnp
from jax import lax
from jax.experimental import pallas as pl
from jax.experimental.pallas import tpu as pltpu
from jax.sharding import PartitionSpec as P


JOINT_BRANCHES = 128


def rotate_kernel(coupling_ref, wannier_ref, partner_ref, out_ref):
    qpoints, points, modes, bands, width = coupling_ref.shape
    half = width // 2

    def rotate_point(point, carry):
        real = wannier_ref[point, :, :half]
        imag = wannier_ref[point, :, half:]
        factor = jnp.concatenate(
            [
                jnp.concatenate([real, imag, imag, -real], axis=1),
                jnp.concatenate([-imag, real, real, imag], axis=1),
            ],
            axis=0,
        )
        for qpoint in range(qpoints):
            block = coupling_ref[qpoint, point].reshape(modes * bands, width)
            turned = jnp.dot(block, factor, preferred_element_type=jnp.float32).astype(jnp.bfloat16)
            partner = partner_ref[qpoint, point]
            partner_rows = jnp.concatenate([partner[:, :half], partner[:, half:]], axis=0)
            stacked = jnp.concatenate(
                [
                    jnp.concatenate(
                        [
                            turned[mode * bands : (mode + 1) * bands, :width],
                            turned[mode * bands : (mode + 1) * bands, width:],
                        ],
                        axis=0,
                    )
                    for mode in range(modes)
                ],
                axis=1,
            )
            rotated = lax.dot_general(
                partner_rows, stacked, (((0,), (0,)), ((), ())), preferred_element_type=jnp.float32
            ).astype(jnp.bfloat16)
            for mode in range(modes):
                out_ref[qpoint, point, mode] = rotated[:, mode * width : (mode + 1) * width]
        return carry

    lax.fori_loop(0, points, rotate_point, 0)


def rotate(coupling, wannier, partner, tile):
    qpoints, points, modes, bands, width = coupling.shape
    return pl.pallas_call(
        rotate_kernel,
        grid=(points // tile,),
        in_specs=[
            pl.BlockSpec((qpoints, tile, modes, bands, width), lambda i: (0, i, 0, 0, 0)),
            pl.BlockSpec((tile, bands, width), lambda i: (i, 0, 0)),
            pl.BlockSpec((qpoints, tile, bands, width), lambda i: (0, i, 0, 0)),
        ],
        out_specs=pl.BlockSpec((qpoints, tile, modes, bands, width), lambda i: (0, i, 0, 0, 0)),
        out_shape=jax.ShapeDtypeStruct(coupling.shape, jnp.bfloat16),
    )(coupling, wannier, partner)


def shift_blocks(block, shift_x, shift_y):
    count_x = lax.axis_size("kx")
    count_y = lax.axis_size("ky")
    pairs = [
        (((x + shift_x) % count_x) * count_y + (y + shift_y) % count_y, x * count_y + y)
        for x in range(count_x)
        for y in range(count_y)
    ]
    return lax.ppermute(block, ("kx", "ky"), pairs)


def fetch(offset_x, shift_y):
    def branch(block):
        rows_x = block.shape[0]
        shift_x, inner_x = divmod(offset_x, rows_x)
        near = shift_blocks(block[inner_x:], shift_x, shift_y)
        if inner_x == 0:
            return near
        far = shift_blocks(block[:inner_x], shift_x + 1, shift_y)
        return jnp.concatenate([near, far], axis=0)

    return branch


def per_device(wannier, coupling, kq_map):
    rows_x, cols_y, bands, width = wannier.shape
    count_y = lax.axis_size("ky")
    total_x = rows_x * lax.axis_size("kx")
    total_y = cols_y * count_y
    qpoints, modes = coupling.shape[0], coupling.shape[3]
    columns = jnp.concatenate([wannier, shift_blocks(wannier, 0, 1)], axis=1)
    joint = total_x * count_y <= JOINT_BRANCHES
    if joint:
        branches = [fetch(x, y) for x in range(total_x) for y in range(count_y)]
    else:
        along_y = [functools.partial(shift_blocks, shift_x=0, shift_y=y) for y in range(count_y)]
        along_x = [fetch(x, 0) for x in range(total_x)]

    def one(carry, offset):
        offset_x, offset_y = offset // total_y, offset % total_y
        aligned = lax.dynamic_slice_in_dim(columns, offset_y % cols_y, cols_y, axis=1)
        shift_y = offset_y // cols_y
        if joint:
            return carry, lax.switch(offset_x * count_y + shift_y, branches, aligned)
        return carry, lax.switch(offset_x, along_x, lax.switch(shift_y, along_y, aligned))

    _, partner = lax.scan(one, 0, kq_map[:, 0])
    points = rows_x * cols_y
    rotated = rotate(
        coupling.reshape(qpoints, points, modes, bands, width),
        wannier.reshape(points, bands, width),
        partner.reshape(qpoints, points, bands, width),
        math.gcd(points, 4),
    )
    return rotated.reshape(coupling.shape)


def solution(mesh):
    in_specs = (P("kx", "ky", None, None), P(None, "kx", "ky", None, None, None), P())
    out_specs = P(None, "kx", "ky", None, None, None)
    return jax.shard_map(
        per_device, mesh=mesh, in_specs=in_specs, out_specs=out_specs, check_vma=False
    )
```

```python
import functools
import math

import jax
import jax.numpy as jnp
from jax import lax
from jax.experimental import pallas as pl
from jax.sharding import PartitionSpec as P


def rotate_kernel(coupling_ref, wannier_ref, *refs):
    partner_refs, out_ref = refs[:-1], refs[-1]
    qpoints, points, modes, bands, width = coupling_ref.shape
    half = width // 2

    def rotate_point(point, carry):
        real = wannier_ref[point, :, :half]
        imag = wannier_ref[point, :, half:]
        factor = jnp.concatenate(
            [jnp.concatenate([real, imag], axis=1), jnp.concatenate([-imag, real], axis=1)], axis=0
        )
        blank = jnp.zeros_like(factor)
        pair_factor = jnp.concatenate(
            [jnp.concatenate([factor, blank], axis=1), jnp.concatenate([blank, factor], axis=1)], axis=0
        )
        blocks = coupling_ref[:, point].reshape(qpoints * modes // 2, 2, bands, width)
        pairs = jnp.concatenate(
            [blocks[:, 0].reshape(-1, width), blocks[:, 1].reshape(-1, width)], axis=1
        )
        turned = jnp.dot(pairs, pair_factor, preferred_element_type=jnp.float32).astype(jnp.bfloat16)
        for qpoint in range(qpoints):
            stacked = []
            for mode in range(modes):
                row, side = divmod(qpoint * modes + mode, 2)
                own = turned[row * bands : (row + 1) * bands, side * width : (side + 1) * width]
                swapped = jnp.concatenate([own[:, half:], -own[:, :half]], axis=1)
                stacked.append(jnp.concatenate([own, swapped], axis=0))
            partner = partner_refs[qpoint][point]
            partner_rows = jnp.concatenate([partner[:, :half], partner[:, half:]], axis=0)
            rotated = lax.dot_general(
                partner_rows,
                jnp.concatenate(stacked, axis=1),
                (((0,), (0,)), ((), ())),
                preferred_element_type=jnp.float32,
            ).astype(jnp.bfloat16)
            for mode in range(modes):
                out_ref[qpoint, point, mode] = rotated[:, mode * width : (mode + 1) * width]
        return carry

    lax.fori_loop(0, points, rotate_point, 0, unroll=points)


def rotate(coupling, wannier, partners, tile):
    qpoints, points, modes, bands, width = coupling.shape
    one_point = pl.BlockSpec((tile, bands, width), lambda i: (i, 0, 0))
    all_modes = pl.BlockSpec((qpoints, tile, modes, bands, width), lambda i: (0, i, 0, 0, 0))
    return pl.pallas_call(
        rotate_kernel,
        grid=(points // tile,),
        in_specs=[all_modes, one_point] + [one_point] * len(partners),
        out_specs=all_modes,
        out_shape=jax.ShapeDtypeStruct(coupling.shape, jnp.bfloat16),
    )(coupling, wannier, *partners)


def shift_blocks(block, shift_x, shift_y):
    count_x = lax.axis_size("kx")
    count_y = lax.axis_size("ky")
    pairs = [
        (((x + shift_x) % count_x) * count_y + (y + shift_y) % count_y, x * count_y + y)
        for x in range(count_x)
        for y in range(count_y)
    ]
    return lax.ppermute(block, ("kx", "ky"), pairs)


def shift_rows(block, offset_x):
    shift_x, inner_x = divmod(offset_x, block.shape[0])
    near = shift_blocks(block[inner_x:], shift_x, 0)
    if inner_x == 0:
        return near
    far = shift_blocks(block[:inner_x], shift_x + 1, 0)
    return jnp.concatenate([near, far], axis=0)


def per_device(wannier, coupling, kq_map):
    rows_x, cols_y, bands, width = wannier.shape
    count_y = lax.axis_size("ky")
    total_x = rows_x * lax.axis_size("kx")
    total_y = cols_y * count_y
    qpoints, modes = coupling.shape[0], coupling.shape[3]
    points = rows_x * cols_y
    columns = jnp.concatenate([wannier, shift_blocks(wannier, 0, 1)], axis=1)
    along_y = [functools.partial(shift_blocks, shift_x=0, shift_y=y) for y in range(count_y)]
    along_x = [functools.partial(shift_rows, offset_x=x) for x in range(total_x)]
    partners = []
    for qpoint in range(qpoints):
        offset_x, offset_y = kq_map[qpoint, 0] // total_y, kq_map[qpoint, 0] % total_y
        aligned = lax.dynamic_slice_in_dim(columns, offset_y % cols_y, cols_y, axis=1)
        aligned = lax.switch(offset_y // cols_y, along_y, aligned)
        partner = lax.switch(offset_x, along_x, aligned)
        partners.append(partner.reshape(points, bands, width))
    rotated = rotate(
        coupling.reshape(qpoints, points, modes, bands, width),
        wannier.reshape(points, bands, width),
        partners,
        math.gcd(points, 4),
    )
    return rotated.reshape(coupling.shape)


def solution(mesh):
    in_specs = (P("kx", "ky", None, None), P(None, "kx", "ky", None, None, None), P())
    out_specs = P(None, "kx", "ky", None, None, None)
    return jax.shard_map(
        per_device, mesh=mesh, in_specs=in_specs, out_specs=out_specs, check_vma=False
    )
```
